32 devices in a mesh: grp: 4 (over y, x), row: 8 (over z, core).
Axes of the slice: x: 2, y: 2, z: 4, core: 2. Of those that a mesh axis runs over, the one named last changes fastest.
Arguments:
- tiles: bfloat16 [4, 8, 32, 256, 256], P('grp', 'row'), may hold values from -0.046875 to 0.046875
- tile_rows: int32 [4, 8, 32], P('grp', 'row'), may hold values from 0 to 3, as said below
- tile_cols: int32 [4, 8, 32], P('grp', 'row'), may hold values from 0 to 7, as said below
- live_tiles: int32 [4, 8], P('grp', 'row'), may hold values from 16 to 32, as said below
- dual_shift: float32 [8192], P('row'), may hold values from 0.5 to 2
- start_block: float32 [32, 8192], P(None, 'row'), may hold values from -6 to 6
Outputs:
- projections: float32 [4, 32, 128], replicated
- factors: float32 [4, 32, 32], replicated
- next_block: float32 [32, 8192], P(None, 'row')
The draws below stay inside these ranges and needn't reach their ends.
Inputs may be any that keep to these rules, and one draw needn't show every extreme that they name: `tile_rows`: the tile slots of one device sit at distinct positions (block row, column block), padding slots included. `tile_cols`: column block j of group g is global block column (j // 1) * 4 + g * 1 + j % 1. Slots from live_tiles on are padding with arbitrary values; in every draw some device has all 32 slots live.
All inputs are finite; a program needn't handle non-finite values.
Results may differ from the reference program's by a relative error of at most 0.013.
Values may be sent and summed in bfloat16 or wider, within the bound.
A program may use at most 64 MiB of HBM per device.

```python
import math
import jax
import jax.numpy as jnp
from jax import lax

K = 32
BS = 256
BR_DEV = 4
KB = 32
ITERS = 4
N = 8192
QB = 1
NCG = 8
M = 128
N_GRP = 4
N_ROW = 8


def tile_slots(key):
    keys = jax.random.split(jax.random.fold_in(key, 7), N_GRP * N_ROW)
    slots = jax.vmap(lambda one_key: jax.random.permutation(one_key, BR_DEV * NCG)[:KB])(keys)
    return slots.reshape(N_GRP, N_ROW, KB).astype(jnp.int32)


def draw_tile_rows(key, part):
    return (tile_slots(key) // NCG).astype(jnp.int32)


def draw_tile_cols(key, part):
    return (tile_slots(key) % NCG).astype(jnp.int32)


def draw_live_tiles(key, part):
    count_key = jax.random.fold_in(key, 11)
    pick_key = jax.random.fold_in(key, 13)
    counts = jax.random.randint(count_key, (N_GRP * N_ROW,), KB // 2, KB + 1)
    picked = jax.random.randint(pick_key, (), 0, N_GRP * N_ROW)
    counts = jnp.where(jnp.arange(N_GRP * N_ROW) == picked, KB, counts)
    return counts.reshape(N_GRP, N_ROW).astype(jnp.int32)


def steps_of(own_key, shape, pieces, low, largest):
    level = 1.0
    for dim, shards_of in pieces:
        heights = jax.random.uniform(jax.random.fold_in(jax.random.fold_in(own_key, 6), dim), (shards_of,), jnp.float32, low / len(pieces), largest / len(pieces))
        level = level * jnp.repeat(jnp.exp(heights), shape[dim] // shards_of).reshape((-1,) + (1,) * (len(shape) - 1 - dim))
    return level


def noise(key, shape, width, reach, shards=(), dtype=jnp.bfloat16):
    array = jax.random.normal(key, shape, jnp.float32) * width
    if len(shards) > 0:
        array = steps_of(key, shape, shards, -0.22, 0.18) * array
    return jnp.clip(array, min=-reach, max=reach).astype(dtype)


def setup_inputs(seed: int = 0) -> dict:
    seeds = jax.random.split(jax.random.key(seed), 7)
    return {
        "tiles": noise(seeds[0], (N_GRP, N_ROW, KB, BS, BS), (KB * N_GRP * 2 * BS // BR_DEV) ** -0.5, 0.046875, ((0, 4), (1, 8))),
        "tile_rows": draw_tile_rows(jax.random.fold_in(seeds[6], 71), 0),
        "tile_cols": draw_tile_cols(jax.random.fold_in(seeds[6], 71), 0),
        "live_tiles": draw_live_tiles(jax.random.fold_in(seeds[6], 71), 0),
        "dual_shift": jnp.clip(jnp.exp(math.log(2.0) - 1.3862944 * jax.random.uniform(seeds[4], (N,), jnp.float32) ** steps_of(seeds[4], (N,), ((0, 8),), -0.2, 0.2)), 0.5, 2.0),
        "start_block": noise(seeds[5], (K, N), 1.0, 6.0, ((1, 8),), jnp.float32),
    }


def inner_product(left, right):
    return lax.dot_general(left.astype(jnp.float32), right.astype(jnp.float32), (((1,), (1,)), ((), ())), precision=lax.Precision.HIGHEST, preferred_element_type=jnp.float32)

def apply_matrix(left, right):
    return jnp.dot(left.astype(jnp.float32), right.astype(jnp.float32), precision=lax.Precision.HIGHEST, preferred_element_type=jnp.float32)

def operate(vectors, tiles, tile_rows, tile_cols, live_tiles):
    rounded = vectors.astype(jnp.bfloat16).astype(jnp.float32).reshape(K, N_ROW, BR_DEV, BS)

    def visit(device, totals):
        direct_sum, back_sum = totals
        group = (device // N_ROW).astype(jnp.int32)
        owner = (device % N_ROW).astype(jnp.int32)
        matrix = tiles[group, owner].astype(jnp.float32)
        rows_here = tile_rows[group, owner]
        cols_here = tile_cols[group, owner]
        live_mask = (jnp.arange(KB) < live_tiles[group, owner]).astype(jnp.float32)
        column_part = lax.dynamic_slice_in_dim(rounded, group * QB, QB, 2).reshape(K, NCG, BS)
        own_part = lax.dynamic_index_in_dim(rounded, owner, 1, False)
        forward = jnp.einsum('kbc,brc->kbr', column_part[:, cols_here], matrix)
        row_table = (rows_here[:, None] == jnp.arange(BR_DEV)[None, :]).astype(jnp.float32) * live_mask[:, None]
        direct = jnp.einsum('kbr,bi->kir', forward, row_table)
        backward = jnp.einsum('kbr,brc->kbc', own_part[:, rows_here], matrix)
        col_table = (cols_here[:, None] == jnp.arange(NCG)[None, :]).astype(jnp.float32) * live_mask[:, None]
        spread = jnp.einsum('kbc,bj->kjc', backward, col_table).reshape(K, N_ROW, QB, BS)
        old_direct = lax.dynamic_index_in_dim(direct_sum, owner, 1, False)
        direct_sum = lax.dynamic_update_index_in_dim(direct_sum, old_direct + direct, owner, 1)
        old_back = lax.dynamic_index_in_dim(back_sum, group, 2, False)
        back_sum = lax.dynamic_update_index_in_dim(back_sum, old_back + spread, group, 2)
        return (direct_sum, back_sum)
    begin = (jnp.zeros((K, N_ROW, BR_DEV, BS), jnp.float32), jnp.zeros((K, N_ROW, N_GRP, QB, BS), jnp.float32))
    direct_sum, back_sum = lax.fori_loop(0, N_GRP * N_ROW, visit, begin)
    return 0.5 * (direct_sum.reshape(K, N) + back_sum.reshape(K, N))

def orthonormal(block):
    lower_factor = jnp.linalg.cholesky(inner_product(block, block))
    return (lax.linalg.triangular_solve(lower_factor, block, left_side=True, lower=True), lower_factor)

def reference(tiles, tile_rows, tile_cols, live_tiles, dual_shift, start_block):
    current, unused = orthonormal(start_block)
    basis_rows = jnp.zeros((M, N), jnp.float32)
    proj_list = []
    factor_list = []
    for step_index in range(ITERS):
        basis_rows = basis_rows.at[step_index * K:(step_index + 1) * K].set(current)
        image = operate(current, tiles, tile_rows, tile_cols, live_tiles) - current * dual_shift[None, :]
        first_coef = inner_product(image, basis_rows)
        image = image - apply_matrix(first_coef, basis_rows)
        current, lower_factor = orthonormal(image)
        proj_list.append(first_coef)
        factor_list.append(lower_factor)
    return (jnp.stack(proj_list), jnp.stack(factor_list), current)
```

```python
import functools

import jax
import jax.numpy as jnp
from jax import lax
from jax.experimental import pallas as pl
from jax.experimental.pallas import tpu as pltpu
from jax.sharding import PartitionSpec as P

ITERS = 4
MESH = pl.DeviceIdType.MESH
HIGH = lax.Precision.HIGHEST
NT = (((1,), (1,)), ((), ()))


def dot_nt(a, b):
    return lax.dot_general(a, b, NT, precision=HIGH, preferred_element_type=jnp.float32)


def dot_nn(a, b):
    return jnp.dot(a, b, precision=HIGH, preferred_element_type=jnp.float32)


def factor_and_inverse(gram):
    n = gram.shape[0]
    row = lax.broadcasted_iota(jnp.int32, (n, 2 * n), 0)
    lane = lax.broadcasted_iota(jnp.int32, (n, 2 * n), 1)
    work = jnp.concatenate([gram, jnp.where(row == lane, 1.0, 0.0)[:, :n]], axis=1)
    lower = jnp.zeros((n, n), jnp.float32)
    pivots = jnp.zeros((n, 2 * n), jnp.float32)
    for k in range(n):
        column = jnp.broadcast_to(work[:, k : k + 1], (n, 2 * n))
        pivot_row = work[k : k + 1, :]
        pivot = column[k : k + 1, :]
        scale = 1.0 / pivot
        below = jnp.where(row > k, column, 0.0)
        lower = jnp.where((lane[:, :n] == k) & (row[:, :n] >= k), column[:, :n] * lax.rsqrt(pivot[:, :n]), lower)
        pivots = jnp.where(row == k, pivot, pivots)
        work = work - below * (pivot_row * scale)
    inverse = (work * lax.rsqrt(pivots))[:, n:]
    return lower, inverse


def kernel(
    steps, group_count, owner_count,
    start_ref, shift_ref, place_ref, tiles_ref,
    proj_ref, fac_ref, next_ref,
    dense, gathered, own, back_out, back_in, direct_out, direct_in,
    dots_grp, dots_row, basis, current, last,
    gather_row_send, gather_row_recv, gather_grp_send, gather_grp_recv,
    back_send, back_recv, direct_send, direct_recv,
    dgrp_send, dgrp_recv, drow_send, drow_recv, last_send, last_recv,
):
    g = lax.axis_index("grp")
    r = lax.axis_index("row")
    width = start_ref.shape[0]
    row_count = start_ref.shape[1]
    part = row_count // group_count
    edge = tiles_ref.shape[1]
    owned = row_count // edge
    per_part = part // edge
    row_peers = [lax.rem(r + d, owner_count) for d in range(1, owner_count)]
    grp_peers = [lax.rem(g + d, group_count) for d in range(1, group_count)]

    barrier = pltpu.get_barrier_semaphore()
    for peer in row_peers:
        pl.semaphore_signal(barrier, inc=1, device_id=(g, peer), device_id_type=MESH)
    for peer in grp_peers:
        pl.semaphore_signal(barrier, inc=1, device_id=(peer, r), device_id_type=MESH)
    pl.semaphore_wait(barrier, len(row_peers) + len(grp_peers))

    def to_row(peer, src, dst, send, recv):
        return pltpu.make_async_remote_copy(
            src_ref=src, dst_ref=dst, send_sem=send, recv_sem=recv,
            device_id=(g, peer), device_id_type=MESH,
        )

    def to_grp(peer, src, dst, send, recv):
        return pltpu.make_async_remote_copy(
            src_ref=src, dst_ref=dst, send_sem=send, recv_sem=recv,
            device_id=(peer, r), device_id_type=MESH,
        )

    def sum_over_row(value):
        dots_row[r] = value
        sends = []
        for peer in row_peers:
            copy = to_row(peer, dots_row.at[r], dots_row.at[r], drow_send.at[peer], drow_recv.at[r])
            copy.start()
            sends.append(copy)
        for peer in row_peers:
            to_row(peer, dots_row.at[peer], dots_row.at[peer], drow_send.at[peer], drow_recv.at[peer]).wait_recv()
        total = dots_row[0]
        for index in range(1, owner_count):
            total = total + dots_row[index]
        for copy in sends:
            copy.wait_send()
        return total

    def sum_over_grp(value):
        dots_grp[g] = value
        sends = []
        for peer in grp_peers:
            copy = to_grp(peer, dots_grp.at[g], dots_grp.at[g], dgrp_send.at[peer], dgrp_recv.at[g])
            copy.start()
            sends.append(copy)
        for peer in grp_peers:
            to_grp(peer, dots_grp.at[peer], dots_grp.at[peer], dgrp_send.at[peer], dgrp_recv.at[peer]).wait_recv()
        total = dots_grp[0]
        for index in range(1, group_count):
            total = total + dots_grp[index]
        for copy in sends:
            copy.wait_send()
        return total

    fold = 128 // width

    def pack(square):
        height = width // fold
        return jnp.concatenate([square[i * height : (i + 1) * height] for i in range(fold)], axis=1)

    def unpack(packed):
        return jnp.concatenate([packed[:, i * width : (i + 1) * width] for i in range(fold)], axis=0)

    total_cols = steps * width
    start = start_ref[...]
    start_gram = pack(dot_nt(start, start))
    start_sum = sum_over_row(
        jnp.concatenate([jnp.zeros((width, total_cols), jnp.float32), start_gram], axis=0)
    )
    for j in range(owner_count * per_part):
        for i in range(owned):
            slot = place_ref[i * owner_count * per_part + j]
            keep = jnp.where(slot > 0, 1.0, 0.0).astype(jnp.bfloat16)
            tile = tiles_ref[jnp.maximum(slot - 1, 0)]
            dense[
                j // per_part,
                i * edge : (i + 1) * edge,
                (j % per_part) * edge : (j % per_part + 1) * edge,
            ] = tile * keep
    basis[...] = jnp.zeros_like(basis)
    proj_ref[...] = jnp.zeros_like(proj_ref)
    unused, inverse = factor_and_inverse(unpack(start_sum[width:]))
    mine = pl.ds(pl.multiple_of(g * part, part), part)
    current[...] = dot_nn(inverse, start_ref[:, mine])
    shift = shift_ref[:, mine]

    def step_body(step, carry):
        now = current[...]
        basis[pl.ds(pl.multiple_of(step * width, width), width), :] = now
        rounded = now.astype(jnp.bfloat16)
        own[g] = rounded
        gathered[r] = rounded
        sends = []
        for peer in grp_peers:
            copy = to_grp(peer, own.at[g], own.at[g], gather_grp_send.at[peer], gather_grp_recv.at[g])
            copy.start()
            sends.append(copy)
        for peer in row_peers:
            copy = to_row(peer, gathered.at[r], gathered.at[r], gather_row_send.at[peer], gather_row_recv.at[r])
            copy.start()
            sends.append(copy)
        for peer in grp_peers:
            to_grp(peer, own.at[peer], own.at[peer], gather_grp_send.at[peer], gather_grp_recv.at[peer]).wait_recv()
        full = jnp.concatenate([own[i] for i in range(group_count)], axis=1)
        for peer in row_peers:
            back_out[peer] = jnp.dot(full, dense[peer], preferred_element_type=jnp.float32).astype(jnp.bfloat16)
            copy = to_row(peer, back_out.at[peer], back_in.at[r], back_send.at[peer], back_recv.at[r])
            copy.start()
            sends.append(copy)
        total = jnp.dot(full, dense[r], preferred_element_type=jnp.float32)
        for peer in row_peers:
            to_row(peer, gathered.at[peer], gathered.at[peer], gather_row_send.at[peer], gather_row_recv.at[peer]).wait_recv()

        def forward(quarter):
            rows = pl.ds(pl.multiple_of(quarter * part, part), part)
            value = jnp.zeros((width, part), jnp.float32)
            for j in range(owner_count):
                value = value + lax.dot_general(
                    gathered[j], dense[j, rows, :], NT, preferred_element_type=jnp.float32
                )
            return value

        for peer in grp_peers:
            direct_out[peer] = forward(peer).astype(jnp.bfloat16)
            copy = to_grp(peer, direct_out.at[peer], direct_in.at[g], direct_send.at[peer], direct_recv.at[g])
            copy.start()
            sends.append(copy)
        total = total + forward(g)
        for peer in row_peers:
            to_row(peer, back_out.at[peer], back_in.at[peer], back_send.at[peer], back_recv.at[peer]).wait_recv()
            total = total + back_in[peer].astype(jnp.float32)
        for peer in grp_peers:
            to_grp(peer, direct_out.at[peer], direct_in.at[peer], direct_send.at[peer], direct_recv.at[peer]).wait_recv()
            total = total + direct_in[peer].astype(jnp.float32)
        for copy in sends:
            copy.wait_send()
        image = 0.5 * total - now * shift

        dots = dot_nt(image, jnp.concatenate([basis[...], image], axis=0))
        packed = jnp.concatenate([dots[:, :total_cols], pack(dots[:, total_cols:])], axis=0)
        summed = sum_over_row(sum_over_grp(packed))
        first = summed[:width]
        gram = unpack(summed[width:]) - dot_nt(first, first)
        image = image - dot_nn(first, basis[...])
        lower, inverse = factor_and_inverse(gram)
        current[...] = dot_nn(inverse, image)
        proj_ref[step] = first
        fac_ref[step] = lower
        return carry

    lax.fori_loop(0, steps, step_body, 0)

    last[g] = current[...]
    sends = []
    for peer in grp_peers:
        copy = to_grp(peer, last.at[g], last.at[g], last_send.at[peer], last_recv.at[g])
        copy.start()
        sends.append(copy)
    for peer in grp_peers:
        to_grp(peer, last.at[peer], last.at[peer], last_send.at[peer], last_recv.at[peer]).wait_recv()
    for index in range(group_count):
        next_ref[:, index * part : (index + 1) * part] = last[index]
    for copy in sends:
        copy.wait_send()


def per_device(tiles, tile_rows, tile_cols, live_tiles, dual_shift, start_block):
    matrix = tiles[0, 0]
    tile_count, edge = matrix.shape[0], matrix.shape[1]
    width, row_count = start_block.shape
    group_count = lax.axis_size("grp")
    owner_count = lax.axis_size("row")
    owned = row_count // edge
    part = row_count // group_count
    columns = part // edge * owner_count
    total_cols = ITERS * width
    order = jnp.arange(tile_count, dtype=jnp.int32)
    position = tile_rows[0, 0] * columns + tile_cols[0, 0]
    here = (position[None, :] == jnp.arange(owned * columns, dtype=jnp.int32)[:, None]) & (
        order < live_tiles[0, 0]
    )[None, :]
    place = jnp.sum(jnp.where(here, order[None, :] + 1, 0), axis=1).astype(jnp.int32)

    vmem = pl.BlockSpec(memory_space=pltpu.VMEM)
    smem = pl.BlockSpec(memory_space=pltpu.SMEM)
    dma = pltpu.SemaphoreType.DMA
    packed = width + width * width // 128
    grp_sem = dma((group_count,))
    row_sem = dma((owner_count,))
    return pl.pallas_call(
        functools.partial(kernel, ITERS, group_count, owner_count),
        out_shape=(
            jax.ShapeDtypeStruct((ITERS, width, total_cols), jnp.float32),
            jax.ShapeDtypeStruct((ITERS, width, width), jnp.float32),
            jax.ShapeDtypeStruct((width, row_count), jnp.float32),
        ),
        in_specs=[vmem, vmem, smem, vmem],
        out_specs=(vmem, vmem, vmem),
        scratch_shapes=[
            pltpu.VMEM((owner_count, row_count, part), jnp.bfloat16),
            pltpu.VMEM((owner_count, width, part), jnp.bfloat16),
            pltpu.VMEM((group_count, width, part), jnp.bfloat16),
            pltpu.VMEM((owner_count, width, part), jnp.bfloat16),
            pltpu.VMEM((owner_count, width, part), jnp.bfloat16),
            pltpu.VMEM((group_count, width, part), jnp.bfloat16),
            pltpu.VMEM((group_count, width, part), jnp.bfloat16),
            pltpu.VMEM((group_count, packed, total_cols), jnp.float32),
            pltpu.VMEM((owner_count, packed, total_cols), jnp.float32),
            pltpu.VMEM((total_cols, part), jnp.float32),
            pltpu.VMEM((width, part), jnp.float32),
            pltpu.VMEM((group_count, width, part), jnp.float32),
            row_sem, row_sem, grp_sem, grp_sem,
            row_sem, row_sem, grp_sem, grp_sem,
            grp_sem, grp_sem, row_sem, row_sem, grp_sem, grp_sem,
        ],
        compiler_params=pltpu.CompilerParams(
            collective_id=0, has_side_effects=True, vmem_limit_bytes=60 * 1024 * 1024
        ),
    )(start_block, dual_shift[None, :], place, matrix)


def solution(mesh):
    in_specs = (
        P("grp", "row", None, None, None),
        P("grp", "row", None),
        P("grp", "row", None),
        P("grp", "row"),
        P("row"),
        P(None, "row"),
    )
    out_specs = (P(), P(), P(None, "row"))
    return jax.shard_map(
        per_device, mesh=mesh, in_specs=in_specs, out_specs=out_specs, check_vma=False
    )
```

```python
import functools

import jax
import jax.numpy as jnp
from jax import lax
from jax.experimental import pallas as pl
from jax.experimental.pallas import tpu as pltpu
from jax.sharding import PartitionSpec as P

ITERS = 4
MESH = pl.DeviceIdType.MESH
HIGH = lax.Precision.HIGHEST
NT = (((1,), (1,)), ((), ()))


def dot_nt(a, b):
    return lax.dot_general(a, b, NT, precision=HIGH, preferred_element_type=jnp.float32)


def dot_nn(a, b):
    return jnp.dot(a, b, precision=HIGH, preferred_element_type=jnp.float32)


def factor_and_inverse(gram):
    n = gram.shape[0]
    row = lax.broadcasted_iota(jnp.int32, (n, 2 * n), 0)
    lane = lax.broadcasted_iota(jnp.int32, (n, 2 * n), 1)
    work = jnp.concatenate([gram, jnp.where(row == lane, 1.0, 0.0)[:, :n]], axis=1)
    lower = jnp.zeros((n, n), jnp.float32)
    pivots = jnp.zeros((n, 2 * n), jnp.float32)
    for k in range(n):
        column = jnp.broadcast_to(work[:, k : k + 1], (n, 2 * n))
        pivot_row = work[k : k + 1, :]
        pivot = column[k : k + 1, :]
        scale = 1.0 / pivot
        below = jnp.where(row > k, column, 0.0)
        lower = jnp.where((lane[:, :n] == k) & (row[:, :n] >= k), column[:, :n] * lax.rsqrt(pivot[:, :n]), lower)
        pivots = jnp.where(row == k, pivot, pivots)
        work = work - below * (pivot_row * scale)
    inverse = (work * lax.rsqrt(pivots))[:, n:]
    return lower, inverse


def kernel(
    steps, group_count, owner_count,
    start_ref, shift_ref, place_ref, tiles_hbm,
    proj_ref, fac_ref, next_ref,
    tiles_ref, dense, gathered, own, back_out, back_in, direct_out, direct_in,
    pair_out, pair_in, dots_pair, dots_grp, dots_row, basis, images, current, last, tile_sem,
    gather_row_send, gather_row_recv, gather_grp_send, gather_grp_recv,
    back_send, back_recv, direct_send, direct_recv,
    dgrp_send, dgrp_recv, drow_send, drow_recv, last_send, last_recv,
    relay_send, pair_send, pair_recv, dpair_send, dpair_recv,
):
    g = lax.axis_index("grp")
    r = lax.axis_index("row")
    width = start_ref.shape[0]
    row_count = start_ref.shape[1]
    part = row_count // group_count
    edge = tiles_ref.shape[1]
    owned = row_count // edge
    per_part = part // edge
    chips = owner_count // 2
    chip, core = r // 2, lax.rem(r, 2)
    partner = chip * 2 + 1 - core
    chip_peers = [lax.rem(chip + d, chips) for d in range(1, chips)]
    row_peers = [peer * 2 + core for peer in chip_peers] + [partner]
    grp_peers = [lax.rem(g + d, group_count) for d in range(1, group_count)]

    load = pltpu.make_async_copy(tiles_hbm, tiles_ref, tile_sem)
    load.start()
    barrier = pltpu.get_barrier_semaphore()
    for peer in row_peers:
        pl.semaphore_signal(barrier, inc=1, device_id=(g, peer), device_id_type=MESH)
    for peer in grp_peers:
        pl.semaphore_signal(barrier, inc=1, device_id=(peer, r), device_id_type=MESH)
    pl.semaphore_wait(barrier, len(row_peers) + len(grp_peers))

    def to_row(peer, src, dst, send, recv):
        return pltpu.make_async_remote_copy(
            src_ref=src, dst_ref=dst, send_sem=send, recv_sem=recv,
            device_id=(g, peer), device_id_type=MESH,
        )

    def to_grp(peer, src, dst, send, recv):
        return pltpu.make_async_remote_copy(
            src_ref=src, dst_ref=dst, send_sem=send, recv_sem=recv,
            device_id=(peer, r), device_id_type=MESH,
        )

    def send_grp_dots(value):
        dots_grp[g] = value
        sends = []
        for peer in grp_peers:
            copy = to_grp(peer, dots_grp.at[g], dots_grp.at[g], dgrp_send.at[peer], dgrp_recv.at[g])
            copy.start()
            sends.append(copy)
        return sends

    def take_grp_dots():
        for peer in grp_peers:
            to_grp(peer, dots_grp.at[peer], dots_grp.at[peer], dgrp_send.at[peer], dgrp_recv.at[peer]).wait_recv()
        total = dots_grp[0]
        for index in range(1, group_count):
            total = total + dots_grp[index]
        return total

    def send_pair_dots(half, value):
        dots_pair[half, core] = value
        copy = to_row(
            partner, dots_pair.at[half, core], dots_pair.at[half, core], dpair_send, dpair_recv.at[half]
        )
        copy.start()
        return [copy]

    def send_row_dots(half):
        to_row(
            partner, dots_pair.at[half, 1 - core], dots_pair.at[half, 1 - core], dpair_send, dpair_recv.at[half]
        ).wait_recv()
        dots_row[half, chip] = dots_pair[half, 0] + dots_pair[half, 1]
        sends = []
        for peer in chip_peers:
            copy = to_row(
                peer * 2 + core, dots_row.at[half, chip], dots_row.at[half, chip],
                drow_send.at[peer], drow_recv.at[half, chip],
            )
            copy.start()
            sends.append(copy)
        return sends

    def take_row_dots(half):
        for peer in chip_peers:
            to_row(
                peer * 2 + core, dots_row.at[half, peer], dots_row.at[half, peer],
                drow_send.at[peer], drow_recv.at[half, peer],
            ).wait_recv()
        total = dots_row[half, 0]
        for index in range(1, chips):
            total = total + dots_row[half, index]
        return total

    fold = 128 // width

    def pack(square):
        height = width // fold
        return jnp.concatenate([square[i * height : (i + 1) * height] for i in range(fold)], axis=1)

    def unpack(packed):
        return jnp.concatenate([packed[:, i * width : (i + 1) * width] for i in range(fold)], axis=0)

    total_cols = steps * width

    def local_dots(block):
        dots = dot_nt(block, jnp.concatenate([basis[...], block], axis=0))
        return jnp.concatenate([dots[:, :total_cols], pack(dots[:, total_cols:])], axis=0)

    def finish_dots(summed):
        first = summed[:width]
        gram = unpack(summed[width:]) - dot_nt(first, first)
        lower, inverse = factor_and_inverse(gram)
        return first, lower, inverse

    basis[...] = jnp.zeros_like(basis)
    images[...] = jnp.zeros_like(images)
    mine = pl.ds(pl.multiple_of(g * part, part), part)
    current[...] = start_ref[:, mine]
    load.wait()
    for j in range(owner_count * per_part):
        for i in range(owned):
            slot = place_ref[i * owner_count * per_part + j]
            keep = jnp.where(slot > 0, 1.0, 0.0).astype(jnp.bfloat16)
            tile = tiles_ref[jnp.maximum(slot - 1, 0)]
            dense[
                j // per_part,
                i * edge : (i + 1) * edge,
                (j % per_part) * edge : (j % per_part + 1) * edge,
            ] = tile * keep

    def both(value):
        return value[:width] + value[width:]

    def step_body(step, carry):
        half = lax.rem(step, 2)
        block = current[...]
        high = block.astype(jnp.bfloat16)
        rest = (block - high.astype(jnp.float32)).astype(jnp.bfloat16)
        split = jnp.concatenate([high, rest], axis=0)
        own[g] = split
        gathered[half, r] = split
        sends = []
        for peer in grp_peers:
            copy = to_grp(peer, own.at[g], own.at[g], gather_grp_send.at[peer], gather_grp_recv.at[g])
            copy.start()
            sends.append(copy)
        for peer in row_peers:
            copy = to_row(
                peer, gathered.at[half, r], gathered.at[half, r],
                gather_row_send.at[peer], gather_row_recv.at[half, r],
            )
            copy.start()
            sends.append(copy)
        sends += send_grp_dots(local_dots(block))
        for peer in grp_peers:
            to_grp(peer, own.at[peer], own.at[peer], gather_grp_send.at[peer], gather_grp_recv.at[peer]).wait_recv()
        full = jnp.concatenate([own[i] for i in range(group_count)], axis=1)
        for peer in chip_peers + [chip]:
            pair_out[peer] = both(
                jnp.dot(full, dense[peer * 2 + 1 - core], preferred_element_type=jnp.float32)
            )
            copy = to_row(
                partner, pair_out.at[peer], pair_in.at[half, peer], pair_send.at[peer], pair_recv.at[half, peer]
            )
            copy.start()
            sends.append(copy)
        kept = [
            both(jnp.dot(full, dense[peer * 2 + core], preferred_element_type=jnp.float32))
            for peer in chip_peers
        ]

        def take_pair(peer):
            to_row(
                partner, pair_out.at[peer], pair_in.at[half, peer], pair_send.at[peer], pair_recv.at[half, peer]
            ).wait_recv()
            return pair_in[half, peer]

        for peer, value in zip(chip_peers, kept):
            back_out[peer] = value + take_pair(peer)
            copy = to_row(
                peer * 2 + core, back_out.at[peer], back_in.at[half, chip],
                back_send.at[peer], back_recv.at[half, chip],
            )
            copy.start()
            sends.append(copy)
        sends += send_pair_dots(half, take_grp_dots())
        for peer in chip_peers:
            slot = peer * 2 + core
            to_row(
                slot, gathered.at[half, slot], gathered.at[half, slot],
                gather_row_send.at[slot], gather_row_recv.at[half, slot],
            ).wait_recv()
            copy = to_row(
                partner, gathered.at[half, slot], gathered.at[half, slot],
                relay_send.at[peer], gather_row_recv.at[half, slot],
            )
            copy.start()
            sends.append(copy)
        sends += send_row_dots(half)
        total = both(jnp.dot(full, dense[r], preferred_element_type=jnp.float32)) + take_pair(chip)
        for peer in chip_peers + [chip]:
            slot = peer * 2 + 1 - core
            to_row(
                partner, gathered.at[half, slot], gathered.at[half, slot],
                relay_send.at[peer], gather_row_recv.at[half, slot],
            ).wait_recv()

        def forward(quarter):
            rows = pl.ds(pl.multiple_of(quarter * part, part), part)
            value = jnp.zeros((2 * width, part), jnp.float32)
            for j in range(owner_count):
                value = value + lax.dot_general(
                    gathered[half, j], dense[j, rows, :], NT, preferred_element_type=jnp.float32
                )
            return both(value)

        for peer in grp_peers:
            direct_out[peer] = forward(peer)
            copy = to_grp(peer, direct_out.at[peer], direct_in.at[g], direct_send.at[peer], direct_recv.at[g])
            copy.start()
            sends.append(copy)
        total = total + forward(g)

        first, lower, inverse = finish_dots(take_row_dots(half))
        last_step = jnp.maximum(step - 1, 0)
        proj_ref[last_step] = first
        fac_ref[last_step] = lower
        now = dot_nn(inverse, block - dot_nn(first, basis[...]))

        for peer in chip_peers:
            to_row(
                peer * 2 + core, back_out.at[peer], back_in.at[half, peer],
                back_send.at[peer], back_recv.at[half, peer],
            ).wait_recv()
            total = total + back_in[half, peer]
        for peer in grp_peers:
            to_grp(peer, direct_out.at[peer], direct_in.at[peer], direct_send.at[peer], direct_recv.at[peer]).wait_recv()
            total = total + direct_in[peer]
        image = dot_nn(inverse, 0.5 * total - dot_nn(first, images[...]))
        place = pl.ds(pl.multiple_of(step * width, width), width)
        basis[place, :] = now
        images[place, :] = image
        current[...] = image - now * shift_ref[:, mine]
        for copy in sends:
            copy.wait_send()
        return carry

    lax.fori_loop(0, steps, step_body, 0)

    block = current[...]
    sends = send_grp_dots(local_dots(block))
    sends += send_pair_dots(steps % 2, take_grp_dots())
    sends += send_row_dots(steps % 2)
    block_parts = take_row_dots(steps % 2)
    first, lower, inverse = finish_dots(block_parts)
    proj_ref[steps - 1] = first
    fac_ref[steps - 1] = lower
    last[g] = dot_nn(inverse, block - dot_nn(first, basis[...]))
    for peer in grp_peers:
        copy = to_grp(peer, last.at[g], last.at[g], last_send.at[peer], last_recv.at[g])
        copy.start()
        sends.append(copy)
    for peer in grp_peers:
        to_grp(peer, last.at[peer], last.at[peer], last_send.at[peer], last_recv.at[peer]).wait_recv()
    for index in range(group_count):
        next_ref[:, index * part : (index + 1) * part] = last[index]
    for copy in sends:
        copy.wait_send()


def hand_on(proj_in, fac_in, next_in, proj_ref, fac_ref, next_ref):
    proj_ref[...] = proj_in[...]
    fac_ref[...] = fac_in[...]
    next_ref[...] = next_in[...]


def per_device(tiles, tile_rows, tile_cols, live_tiles, dual_shift, start_block):
    matrix = tiles[0, 0]
    tile_count, edge = matrix.shape[0], matrix.shape[1]
    width, row_count = start_block.shape
    group_count = lax.axis_size("grp")
    owner_count = lax.axis_size("row")
    owned = row_count // edge
    part = row_count // group_count
    columns = part // edge * owner_count
    total_cols = ITERS * width
    order = jnp.arange(tile_count, dtype=jnp.int32)
    position = tile_rows[0, 0] * columns + tile_cols[0, 0]
    here = (position[None, :] == jnp.arange(owned * columns, dtype=jnp.int32)[:, None]) & (
        order < live_tiles[0, 0]
    )[None, :]
    place = jnp.sum(jnp.where(here, order[None, :] + 1, 0), axis=1).astype(jnp.int32)

    vmem = pl.BlockSpec(memory_space=pltpu.VMEM)
    smem = pl.BlockSpec(memory_space=pltpu.SMEM)
    dma = pltpu.SemaphoreType.DMA
    packed = width + width * width // 128
    grp_sem = dma((group_count,))
    row_sem = dma((owner_count,))
    row_pair = dma((2, owner_count))
    shapes = (
            jax.ShapeDtypeStruct((ITERS, width, total_cols), jnp.float32),
            jax.ShapeDtypeStruct((ITERS, width, width), jnp.float32),
            jax.ShapeDtypeStruct((width, row_count), jnp.float32),
    )
    outs = pl.pallas_call(
        functools.partial(kernel, ITERS, group_count, owner_count),
        out_shape=shapes,
        in_specs=[vmem, vmem, smem, pl.BlockSpec(memory_space=pl.ANY)],
        out_specs=(vmem, vmem, vmem),
        scratch_shapes=[
            pltpu.VMEM(matrix.shape, jnp.bfloat16),
            pltpu.VMEM((owner_count, row_count, part), jnp.bfloat16),
            pltpu.VMEM((2, owner_count, 2 * width, part), jnp.bfloat16),
            pltpu.VMEM((group_count, 2 * width, part), jnp.bfloat16),
            pltpu.VMEM((owner_count // 2, width, part), jnp.float32),
            pltpu.VMEM((2, owner_count // 2, width, part), jnp.float32),
            pltpu.VMEM((group_count, width, part), jnp.float32),
            pltpu.VMEM((group_count, width, part), jnp.float32),
            pltpu.VMEM((owner_count // 2, width, part), jnp.float32),
            pltpu.VMEM((2, owner_count // 2, width, part), jnp.float32),
            pltpu.VMEM((2, 2, packed, total_cols), jnp.float32),
            pltpu.VMEM((group_count, packed, total_cols), jnp.float32),
            pltpu.VMEM((2, owner_count // 2, packed, total_cols), jnp.float32),
            pltpu.VMEM((total_cols, part), jnp.float32),
            pltpu.VMEM((total_cols, part), jnp.float32),
            pltpu.VMEM((width, part), jnp.float32),
            pltpu.VMEM((group_count, width, part), jnp.float32),
            pltpu.SemaphoreType.DMA,
            row_sem, row_pair, grp_sem, grp_sem,
            row_sem, row_pair, grp_sem, grp_sem,
            grp_sem, grp_sem, row_sem, row_pair, grp_sem, grp_sem,
            row_sem, row_sem, row_pair, dma, dma((2,)),
        ],
        compiler_params=pltpu.CompilerParams(
            collective_id=0, has_side_effects=True, vmem_limit_bytes=60 * 1024 * 1024
        ),
    )(start_block, dual_shift[None, :], place, matrix)
    return pl.pallas_call(hand_on, out_shape=shapes, in_specs=[vmem] * 3, out_specs=(vmem,) * 3)(*outs)


def solution(mesh):
    in_specs = (
        P("grp", "row", None, None, None),
        P("grp", "row", None),
        P("grp", "row", None),
        P("grp", "row"),
        P("row"),
        P(None, "row"),
    )
    out_specs = (P(), P(), P(None, "row"))
    return jax.shard_map(
        per_device, mesh=mesh, in_specs=in_specs, out_specs=out_specs, check_vma=False
    )
```
